32 devices in a mesh: ep: 8 (over z, y), tp: 4 (over x, core).
Axes of the slice: x: 2, y: 2, z: 4, core: 2. Of those that a mesh axis runs over, the one named last changes fastest.
Arguments:
- tokens: bfloat16 [512, 4096], P(('ep', 'tp')), may hold values from -6 to 6
- routes: int32 [512, 2], P(('ep', 'tp')), may hold values from 0 to 7, all different within a row; in each aligned block of 16 rows (0 to 15, 16 to 31, ...) at most 8 rows name the same one
- combine: float32 [512, 2], P(('ep', 'tp')), may hold values from 0.25 to 1
- gate_weight: bfloat16 [8, 4096, 4096], P('ep', None, 'tp'), may hold values from -0.09375 to 0.09375
- up_weight: bfloat16 [8, 4096, 4096], P('ep', None, 'tp'), may hold values from -0.09375 to 0.09375
- down_weight: bfloat16 [8, 4096, 4096], P('ep', 'tp'), may hold values from -0.09375 to 0.09375
Outputs:
- moe_output: bfloat16 [512, 4096], P(('ep', 'tp'))
The draws below stay inside these ranges and needn't reach their ends.
Inputs may be any that keep to these rules, and one draw needn't show every extreme that they name: `routes`: each row names 2 different experts. Among the rows of one device no expert is named more than 8 times, and in every draw some expert is named exactly 8 times by the rows of some device.
All inputs are finite; a program needn't handle non-finite values.
Results may differ from the reference program's by a relative error of at most 0.015.
Values may be sent and summed in bfloat16 or wider, within the bound.
No kernel may reach another device: no remote copies, remote signals or barrier semaphores. Data moves between devices by JAX's collectives and lax.ppermute only.
A program may use at most 64 MiB of HBM per device.

```python
import math
import jax
import jax.numpy as jnp
import numpy as np
from jax import lax

D = 4096
FF = 4096
TOP = 2
TOK_DEV = 16
E = 8
FF_DEV = 1024
C = 8
TOKENS = 512
N_TP = 4
DEVICES = 32


def block_scale(rng, dims, split, smallest, top_value):
    def one(dim, parts):
        steps = jax.random.uniform(jax.random.fold_in(jax.random.fold_in(rng, 6), dim), (parts,), jnp.float32, smallest / len(split), top_value / len(split))
        return jnp.repeat(jnp.exp(steps), dims[dim] // parts).reshape((-1,) + (1,) * (len(dims) - dim - 1))

    gain = one(*split[0])
    for cut in split[1:]:
        gain = gain * one(*cut)
    return gain


def assign_block(stream_key, own, number, rows, number_of, top, bound, slope):
    ranking = jax.random.permutation(stream_key, number_of)
    crowded, common = shares(number_of, rows * top, bound, slope, True), shares(number_of, rows * top, bound, slope, False)
    places = jnp.arange(number_of)

    def named(sizes, offset_by):
        used = int((sizes > 0).sum())
        fixed = max(1, used // 4)
        shifted = fixed + (places - fixed + offset_by * (used - fixed)) % max(1, number_of - fixed)
        return jnp.zeros((number_of,), jnp.int32).at[ranking[jnp.where(places < fixed, places, shifted)]].set(jnp.asarray(sizes, jnp.int32))

    sizes = jnp.where(number % 4 == 0, named(crowded, number // 4), named(common, number - number // 4 - 1))
    mixed = jax.random.permutation(jax.random.fold_in(own, 3), number_of)
    giver, sink = mixed[0:number_of // 2 * 2:2], mixed[1:number_of // 2 * 2:2]
    slack = jnp.minimum(sizes[giver] - 1, bound - sizes[sink]) // 2
    slack = jnp.where((giver == ranking[0]) | (sink == ranking[0]) | (sizes[sink] == 0), 0, jnp.maximum(slack, 0))
    shifted = jax.random.randint(jax.random.fold_in(own, 4), (number_of // 2,), 0, 1 << 20) % (slack + 1)
    sizes = sizes.at[giver].add(-shifted).at[sink].add(shifted)
    items = jnp.searchsorted(jnp.cumsum(sizes), jnp.arange(rows * top), side="right").astype(jnp.int32)
    table = items.reshape(top, rows).T
    table = table[jax.random.permutation(jax.random.fold_in(own, 1), rows)]
    offset_by = jax.random.randint(jax.random.fold_in(own, 2), (rows, 1), 0, top)
    return jnp.take_along_axis(table, (jnp.arange(top)[None, :] + offset_by) % top, axis=1)


def shares(number_of, total, bound, skew, full):
    loads = [(1 << 20) // math.isqrt(grade ** skew) + 1 for grade in range(1, number_of + 1)]
    largest = bound if full else min(bound, max(-(-total // number_of), total * loads[0] // sum(loads)))
    least = 1 if total - largest >= number_of - 1 else 0
    holding, surplus = [largest] + [least] * (number_of - 1), total - largest - least * (number_of - 1)
    while surplus > 0:
        candidates = [i for i in range(1, number_of) if holding[i] < largest] or [i for i in range(1, number_of) if holding[i] < bound]
        pool, remaining = sum([loads[i] for i in candidates]), surplus
        for i in candidates:
            addition = min(bound - holding[i], max(1, remaining * loads[i] // pool), surplus)
            holding[i] = holding[i] + addition
            surplus = surplus - addition
    return np.array(holding)


def centred(stream_key, shape, width, bound, split=(), kind=jnp.bfloat16):
    drawn = jax.random.normal(stream_key, shape, jnp.float32) * width
    if len(split) > 0:
        drawn = block_scale(stream_key, shape, split, -0.22, 0.18) * drawn
    return jnp.clip(drawn, min=-bound, max=bound).astype(kind)


def setup_inputs(seed: int = 0) -> dict:
    splits = jax.random.split(jax.random.key(seed), 7)
    tokens = centred(splits[0], (TOKENS, D), 1.0, 6.0, ((0, 32),))
    routes_keys = jax.random.split(jax.random.fold_in(splits[1], 1), TOKENS // TOK_DEV)
    routes_turns = jax.random.permutation(jax.random.fold_in(splits[1], 3), TOKENS // TOK_DEV)
    routes = jax.vmap(lambda own, number: assign_block(jax.random.fold_in(splits[1], 2), own, number, TOK_DEV, E, TOP, C, 2))(routes_keys, routes_turns).reshape((TOKENS, TOP))
    combine = jnp.clip(0.25 + 0.75 * jax.random.uniform(splits[2], (TOKENS, TOP), jnp.float32) ** block_scale(splits[2], (TOKENS, TOP), ((0, 32),), -0.2, 0.2), 0.25, 1.0)
    gate_weight = centred(splits[3], (E, D, FF), D ** -0.5, 0.09375, ((0, 8), (2, 4)))
    up_weight = centred(splits[4], (E, D, FF), D ** -0.5, 0.09375, ((0, 8), (2, 4)))
    down_weight = centred(splits[5], (E, FF, D), FF ** -0.5, 0.09375, ((0, 8), (1, 4)))
    return dict(tokens=tokens, routes=routes, combine=combine, gate_weight=gate_weight, up_weight=up_weight, down_weight=down_weight)


def reference(tokens, routes, combine, gate_weight, up_weight, down_weight):
    assignments = TOK_DEV * TOP
    flat_ids = routes.reshape(DEVICES, assignments).astype(jnp.int32)
    onehot = (flat_ids[:, :, None] == jnp.arange(E, dtype=jnp.int32)[None, None, :]).astype(jnp.int32)
    earlier = jnp.cumsum(onehot, axis=1) - onehot
    slot_index = jnp.sum(earlier * onehot, axis=2)
    target = flat_ids * C + slot_index
    selector = (target[:, :, None] == jnp.arange(E * C, dtype=jnp.int32)[None, None, :]).astype(jnp.float32)
    repeated = jnp.repeat(tokens.reshape(DEVICES, TOK_DEV, D), TOP, axis=1).astype(jnp.float32)
    buffer = jnp.einsum("sak,sad->skd", selector, repeated, precision=lax.Precision.HIGHEST).astype(jnp.bfloat16)
    buffer = buffer.reshape(DEVICES, E, C, D).transpose(1, 0, 2, 3).reshape(E, DEVICES * C, D)

    def expert(operands):
        inputs, w_gate, w_up, w_down = operands
        gate_values = jnp.dot(inputs, w_gate, preferred_element_type=jnp.float32)
        up_values = jnp.dot(inputs, w_up, preferred_element_type=jnp.float32)
        hidden = (jax.nn.silu(gate_values) * up_values).astype(jnp.bfloat16)
        hidden_split = hidden.reshape(DEVICES * C, N_TP, FF_DEV).astype(jnp.float32)
        down_split = w_down.reshape(N_TP, FF_DEV, D).astype(jnp.float32)
        group_parts = jnp.einsum("rgf,gfd->grd", hidden_split, down_split, precision=lax.Precision.HIGHEST).astype(jnp.bfloat16)
        return jnp.sum(group_parts.astype(jnp.float32), axis=0).astype(jnp.bfloat16)

    expert_results = lax.map(expert, (buffer, gate_weight, up_weight, down_weight))
    returned = expert_results.reshape(E, DEVICES, C, D).transpose(1, 0, 2, 3).reshape(DEVICES, E * C, D).astype(jnp.float32)
    picked = jnp.einsum("sak,skd->sad", selector, returned, precision=lax.Precision.HIGHEST).reshape(TOKENS, TOP, D)
    return jnp.sum(combine[:, :, None] * picked, axis=1).astype(jnp.bfloat16)
```

```python
import jax
import jax.numpy as jnp
from jax import lax
from jax.experimental import pallas as pl
from jax.experimental.pallas import tpu as pltpu
from jax.sharding import PartitionSpec as P

VMEM = pl.BlockSpec(memory_space=pltpu.VMEM)


def call(kernel, outs, ins, scratch=(), limit=8 << 20, name=None):
    return pl.pallas_call(
        kernel,
        out_shape=outs,
        in_specs=[VMEM] * len(ins),
        out_specs=jax.tree.map(lambda _: VMEM, outs),
        scratch_shapes=list(scratch),
        compiler_params=pltpu.CompilerParams(vmem_limit_bytes=limit),
        name=name,
    )(*ins)


def hits(routes, weights, capacity, blocks, me):
    tokens = routes.shape[1]
    slots = blocks * capacity
    row = lax.broadcasted_iota(jnp.int32, (slots, tokens), 0)
    expert = jnp.bitwise_xor(row // capacity, me)
    place = (row % capacity).astype(jnp.float32)
    named = [routes[k : k + 1, :] == expert for k in range(routes.shape[0])]
    member = sum(n.astype(jnp.float32) for n in named)
    older = lax.broadcasted_iota(jnp.int32, (tokens, tokens), 0)
    newer = lax.broadcasted_iota(jnp.int32, (tokens, tokens), 1)
    earlier = jnp.dot(member, (older < newer).astype(jnp.float32), preferred_element_type=jnp.float32)
    here = earlier == place
    value = sum(jnp.where(n, w, 0.0) for n, w in zip(named, weights))
    return jnp.where(here, value, 0.0)


def make_build(blocks, capacity):
    def build(routes_ref, tokens_ref, *outs):
        me = lax.axis_index("ep")
        routes = routes_ref[...]
        chosen = hits(routes, [1.0] * routes.shape[0], capacity, blocks, me).astype(jnp.bfloat16)
        rows = jnp.dot(chosen, tokens_ref[...], preferred_element_type=jnp.float32).astype(jnp.bfloat16)
        for k in range(blocks):
            outs[k][...] = rows[k * capacity : (k + 1) * capacity]

    return build


def make_ffn(group_rows, tile):
    def ffn(*refs):
        count = len(group_rows)
        ins, (gate, up, down), (keep, send), (rows, hidden) = refs[:count], refs[count : count + 3], refs[count + 3 : count + 5], refs[count + 5 :]
        at = 0
        for ref in ins:
            rows[pl.ds(at, ref.shape[0]), :] = ref[...]
            at += ref.shape[0]

        def first(i, _):
            cols = pl.ds(pl.multiple_of(i * tile, tile), tile)
            g = jnp.dot(rows[...], gate[0, :, cols], preferred_element_type=jnp.float32)
            u = jnp.dot(rows[...], up[0, :, cols], preferred_element_type=jnp.float32)
            hidden[:, cols] = (g / (1.0 + jnp.exp(-g)) * u).astype(jnp.bfloat16)
            return 0

        lax.fori_loop(0, gate.shape[2] // tile, first, 0)
        half = keep.shape[0]

        def second(i, _):
            cols = pl.ds(pl.multiple_of(i * tile, tile), tile)
            p = jnp.dot(hidden[...], down[0, :, cols], preferred_element_type=jnp.float32).astype(jnp.bfloat16)
            keep[:, cols] = p[:half]
            send[:, cols] = p[half:]
            return 0

        lax.fori_loop(0, down.shape[2] // tile, second, 0)

    return ffn


def make_combine(blocks, capacity):
    def finish(routes_ref, combine_ref, *refs):
        ins, out, rows = refs[:blocks], refs[blocks], refs[blocks + 1]
        me = lax.axis_index("ep")
        combine = combine_ref[...]
        weights = [combine[k : k + 1, :] for k in range(combine.shape[0])]
        w = hits(routes_ref[...], weights, capacity, blocks, me)
        for k in range(blocks):
            rows[pl.ds(k * capacity, capacity), :] = ins[k][...]
        high = w.astype(jnp.bfloat16)
        low = (w - high.astype(jnp.float32)).astype(jnp.bfloat16)
        dims = (((0,), (0,)), ((), ()))
        y = lax.dot_general(high, rows[...], dims, preferred_element_type=jnp.float32)
        y += lax.dot_general(low, rows[...], dims, preferred_element_type=jnp.float32)
        out[...] = y.astype(jnp.bfloat16)

    return finish


def make_body(ep, tp):
    chips = tp // 2

    def over_ep(x, k):
        return lax.ppermute(x, "ep", [(i, i ^ k) for i in range(ep)])

    def over_tp(x, k):
        return lax.ppermute(x, "tp", [(i, i ^ k) for i in range(tp)])

    def body(tokens, routes, combine, gate_weight, up_weight, down_weight):
        token_rows, width = tokens.shape
        top = routes.shape[1]
        capacity = 2 * token_rows * top // ep
        bf16 = jnp.bfloat16
        block = jax.ShapeDtypeStruct((capacity, width), bf16)
        slots = call(make_build(ep, capacity), [block] * ep, (routes.T, tokens), name="build")
        mine = [slots[0]] + [over_ep(slots[k], k) for k in range(1, ep)]
        wide = [[over_tp(r, 2 * j) for r in mine] for j in range(1, chips)]
        half = mine + [r for w in wide for r in w]
        other = [over_tp(r, 1) for r in half]
        ins = half + other
        rows = len(half) * capacity
        part = jax.ShapeDtypeStruct((rows, width), bf16)
        keep, send = call(
            make_ffn([r.shape[0] for r in ins], 256),
            [part, part],
            (*ins, gate_weight, up_weight, down_weight),
            [pltpu.VMEM((2 * rows, width), bf16), pltpu.VMEM((2 * rows, gate_weight.shape[2]), bf16)],
            limit=20 << 20,
            name="ffn",
        )
        got = over_tp(send, 1)
        pair = (keep.astype(jnp.float32) + got.astype(jnp.float32)).reshape(chips, ep, capacity, width)
        back = []
        for k in range(ep):
            total = pair[0, k]
            for j in range(1, chips):
                total = total + over_tp(pair[j, k].astype(bf16), 2 * j).astype(jnp.float32)
            total = total.astype(bf16)
            back.append(over_ep(total, k) if k else total)
        return call(
            make_combine(ep, capacity),
            jax.ShapeDtypeStruct((token_rows, width), bf16),
            (routes.T, combine.T, *back),
            [pltpu.VMEM((ep * capacity, width), bf16)],
            name="finish",
        )

    return body


def solution(mesh):
    return jax.shard_map(
        make_body(mesh.shape["ep"], mesh.shape["tp"]),
        mesh=mesh,
        in_specs=(
            P(("ep", "tp"), None),
            P(("ep", "tp"), None),
            P(("ep", "tp"), None),
            P("ep", None, "tp"),
            P("ep", None, "tp"),
            P("ep", "tp", None),
        ),
        out_specs=P(("ep", "tp"), None),
        check_vma=False,
    )
```
